32 devices in a mesh: rows: 2 (over x), cols: 4 (over z), slabs: 2 (over y), trial: 2 (over core).
Axes of the slice: x: 2, y: 2, z: 4, core: 2. Of those that a mesh axis runs over, the one named last changes fastest.
Arguments:
- field_values: float32 [32, 64, 128, 128], P(('trial', 'rows'), 'cols', 'slabs'), parts along dimension 0, may hold values from 0.2 to 1.8
- crowding: float32 [32, 64, 128, 128], P(('trial', 'rows'), 'cols', 'slabs'), parts along dimension 0, may hold values from 0.5 to 2
Outputs:
- potential: float32 [32, 64, 128, 128], P(('trial', 'rows'), 'cols', 'slabs'), parts along dimension 0
- field_values_end: float32 [32, 64, 128, 128], P(('trial', 'rows'), 'cols', 'slabs'), parts along dimension 0
The draws below stay inside these ranges and needn't reach their ends.
There are 2 independent parts, one for each index of `trial`. The reference program is written for one: setup_inputs(seed, part) draws one part's arguments, and reference() takes and returns one part's arrays. A program takes and returns all parts, laid end to end along the dimension named above; each array names one. Nothing has to cross between parts.
All inputs are finite; a program needn't handle non-finite values.
Results may differ from the reference program's by a relative error of at most 0.00002.
Values sent between devices are 32-bit elements; how exact they have to be, the bound alone decides.
A program may use at most 64 MiB of HBM per device.

```python
import jax
import jax.numpy as jnp
from jax import lax

GRID_J = 16
GRID_I = 64
GRID_K = 128
LEVELS = 128
STEPS = 3


def block_levels(rng, shape, pieces, least, top_value):
    factor_of = 1.0
    for axis_at, parts in pieces:
        steps = jax.random.uniform(jax.random.fold_in(jax.random.fold_in(rng, 6), axis_at), (parts,), jnp.float32, least / len(pieces), top_value / len(pieces))
        factor_of = factor_of * jnp.repeat(jnp.exp(steps), shape[axis_at] // parts).reshape((-1,) + (1,) * (len(shape) - 1 - axis_at))
    return factor_of


def setup_inputs(seed: int = 0, part: int = 0) -> dict:
    keys = jax.random.split(jax.random.key(seed), 3)
    part_splits = jax.random.split(jax.random.fold_in(keys[2], part), 3)
    return {
        "field_values": jnp.clip(0.2 + 1.5999999 * jax.random.uniform(part_splits[0], (GRID_J, GRID_I, GRID_K, LEVELS), jnp.float32) ** block_levels(part_splits[0], (GRID_J, GRID_I, GRID_K, LEVELS), ((0, 2), (1, 4), (2, 2)), -0.2, 0.2), 0.2, 1.8),
        "crowding": jnp.clip(0.5 + 1.5 * jax.random.uniform(part_splits[1], (GRID_J, GRID_I, GRID_K, LEVELS), jnp.float32) ** block_levels(part_splits[1], (GRID_J, GRID_I, GRID_K, LEVELS), ((0, 2), (1, 4), (2, 2)), -0.2, 0.2), 0.5, 2.0),
    }


def without_rim(values, dims):
    for dim in dims:
        values = lax.slice_in_dim(values, 1, values.shape[dim] - 1, axis=dim)
    return values


def shifted_cells(values, dim, start, dims):
    others = [other for other in dims if other != dim]
    values = without_rim(values, others)
    return lax.slice_in_dim(values, start, start + values.shape[dim] - 2, axis=dim)


def march_step(padded, crowding):
    middle = without_rim(padded, (0, 1, 2))
    lower = [shifted_cells(padded, dim, 0, (0, 1, 2)) for dim in (0, 1, 2)]
    upper = [shifted_cells(padded, dim, 2, (0, 1, 2)) for dim in (0, 1, 2)]
    spread = lower[0] + upper[0] + lower[1] + upper[1] + lower[2] + upper[2] - 6.0 * middle
    return middle + 0.1 * spread + 0.2 * middle * (1.0 - middle * crowding)


def reference(field_values, crowding):
    for step in range(STEPS):
        field_values = march_step(jnp.pad(field_values, ((1, 1), (1, 1), (1, 1), (0, 0)), mode="constant"), crowding)
    potential = jnp.cumsum(field_values, axis=0) / GRID_J
    return potential, field_values
```

```python
import functools

import jax
import jax.numpy as jnp
from jax import lax
from jax.experimental import pallas as pl
from jax.experimental.pallas import tpu as pltpu
from jax.sharding import PartitionSpec as P

STEPS = 3
MESH = pl.DeviceIdType.MESH
AXES = ("rows", "cols", "slabs")
PAD = 8


def pieces_of(length, counts):
    for count in counts:
        if length % count == 0:
            return count
    return 1


def segments_of(I):
    if I % 4:
        return ((0, I),)
    return ((0, I // 2), (I // 2, I // 4), (I - I // 4, I // 4))


def cut(I, eighths):
    lead = I * eighths // 8 if I % 8 == 0 else I - I // 2
    return ((0, lead), (lead, I - lead))


def loop(low, high, body):
    def step(at, _):
        body(at)
        return 0

    lax.fori_loop(low, high, step, 0)


def march_kernel(sizes, field, crowd, final, *refs):
    segments = segments_of(field.shape[1])
    totals, refs = refs[: len(segments)], refs[len(segments) :]
    (
        grid0, grid1, grid2, cells, x_in, part, y_in, y_out,
        x_send, x_recv, z_send, z_recv, y_send, y_recv, load, go,
    ) = refs
    J, I, K, L = field.shape
    grids = (grid0, grid1, grid2)
    x_parts = [((0, I),)] * (STEPS - 2) + [cut(I, 6), cut(I, 6)]
    x_slot = [step + max(step - STEPS + 2, 0) for step in range(STEPS)]
    U = pieces_of(I, (4, 2))
    inside = pl.ds(PAD, K)
    place = {axis: lax.axis_index(axis) for axis in AXES}
    has_target = {}
    has_source = {}
    for axis in AXES:
        later, earlier = place[axis] < sizes[axis] - 1, place[axis] > 0
        has_target[axis] = (later, earlier)
        has_source[axis] = (earlier, later)
    trial = lax.axis_index("trial")
    first = lax.rem(trial, 2) == 0
    paired = sizes["trial"] % 2 == 0 and sizes["rows"] > 1
    partner = {"trial": trial + 1 - 2 * lax.rem(trial, 2)}
    out_plane = (J - 1, 0)
    in_plane = (0, J - 1)
    out_at = (0, 1)
    in_at = (1, 0)
    rows = ((0, 2), (2, J - 2))

    def target(axis, way):
        n = sizes[axis]
        return {axis: lax.rem(place[axis] + (1 if way == 0 else n - 1), n)}

    load_field = [
        pltpu.make_async_copy(
            field.at[: J - 1], grid0.at[1:J, 1 : I + 1, inside], load.at[0]
        ),
        pltpu.make_async_copy(
            field.at[J - 1], grid0.at[0, 1 : I + 1, inside], load.at[1]
        ),
    ]
    load_cells = pltpu.make_async_copy(crowd, cells, load.at[2])
    for one in load_field:
        one.start()
    load_cells.start()

    barrier = pltpu.get_barrier_semaphore()
    peers = jnp.int32(1 if paired else 0)
    for axis in AXES:
        if sizes[axis] > 1:
            for way in (0, 1):

                @pl.when(has_target[axis][way])
                def _():
                    pl.semaphore_signal(
                        barrier, inc=1, device_id=target(axis, way), device_id_type=MESH
                    )

                peers = peers + has_source[axis][way].astype(jnp.int32)
    if paired:
        pl.semaphore_signal(barrier, inc=1, device_id=partner, device_id_type=MESH)
    pl.semaphore_wait(barrier, peers)

    def x_copy(step, way, n):
        at, count = x_parts[step][n]
        columns = pl.ds(at, count)
        if step == 0:
            source = field.at[out_plane[way], columns]
        else:
            source = part.at[step - 1, way, columns]
        return pltpu.make_async_remote_copy(
            src_ref=source,
            dst_ref=x_in.at[step, way, columns],
            send_sem=x_send.at[x_slot[step] + n, way],
            recv_sem=x_recv.at[x_slot[step] + n, way],
            device_id=target("rows", way),
            device_id_type=MESH,
        )

    def z_copy(step, way, piece):
        column = I - 1 if way == 0 else 0
        halo = 0 if way == 0 else I + 1
        if step == 0:
            at, count = ((0, 1), (1, J - 1))[piece]
            source = field.at[pl.ds((J - 1, 0)[piece], count), column]
        else:
            at, count = rows[piece]
            source = grids[step].at[pl.ds(at, count), 1 + column, inside]
        return pltpu.make_async_remote_copy(
            src_ref=source,
            dst_ref=grids[step].at[pl.ds(at, count), halo, inside],
            send_sem=z_send.at[way, piece],
            recv_sem=z_recv.at[step, way, piece],
            device_id=target("cols", way),
            device_id_type=MESH,
        )

    def y_copy(step, way, piece):
        at, count = rows[piece]
        return pltpu.make_async_remote_copy(
            src_ref=y_out.at[step, 1 - way, pl.ds(at, count)],
            dst_ref=y_in.at[step, way, pl.ds(at, count)],
            send_sem=y_send.at[way, piece],
            recv_sem=y_recv.at[step, way, piece],
            device_id=target("slabs", way),
            device_id_type=MESH,
        )

    def start(axis, way, copies):
        if sizes[axis] > 1:

            @pl.when(has_target[axis][way])
            def _():
                for one in copies:
                    one.start()

    def sent(axis, way, copies):
        if sizes[axis] > 1:

            @pl.when(has_target[axis][way])
            def _():
                for one in copies:
                    one.wait_send()

    def arrived(axis, way, copies):
        if sizes[axis] > 1:

            @pl.when(has_source[axis][way])
            def _():
                for one in copies:
                    one.wait_recv()

    def send_rims(step, pieces):
        for way in (0, 1):
            if step > 0:
                sent("slabs", way, [y_copy(step - 1, way, piece) for piece in pieces])
            start("slabs", way, [y_copy(step, way, piece) for piece in pieces])

    def send_columns(step, pieces):
        for way in (0, 1):
            if step > 0:
                sent("cols", way, [z_copy(step - 1, way, piece) for piece in pieces])
            start("cols", way, [z_copy(step, way, piece) for piece in pieces])

    def receive(step, pieces):
        grid = grids[step]
        for way in (0, 1):
            arrived("slabs", way, [y_copy(step, way, piece) for piece in pieces])
            row = PAD - 1 if way == 0 else PAD + K

            def place_row(j):
                def body(i):
                    for u in range(U):
                        at = i * U + u
                        grid[j, 1 + at, pl.ds(row, 1), :] = y_in[
                            step, way, j, pl.ds(at, 1), :
                        ]

                loop(0, I // U, body)

            @pl.when(has_source["slabs"][way])
            def _():
                for piece in pieces:
                    at, count = rows[piece]
                    loop(at, at + count, place_row)

        for way in (0, 1):
            arrived("cols", way, [z_copy(step, way, piece) for piece in pieces])

    def keep_rims(step, j):
        def body(i):
            for u in range(U):
                at = i * U + u
                for side, row in ((0, PAD), (1, PAD + K - 1)):
                    y_out[step, side, j, pl.ds(at, 1), :] = grids[step][
                        j, 1 + at, pl.ds(row, 1), :
                    ]

        loop(0, I // U, body)

    def tile(step, j, at, i, beside):
        old = grids[step - 1]
        middle = old[at, 1 + i, inside]
        around = (old[at, i, inside] + old[at, 2 + i, inside]) + (
            old[at, 1 + i, pl.ds(PAD - 1, K)] + old[at, 1 + i, pl.ds(PAD + 1, K)]
        )
        for other in beside:
            around = around + old[other, 1 + i, inside]
        return middle * (0.6 - 0.2 * (middle * cells[j, i])) + 0.1 * around

    def interior(step, low, high):
        def row(j):
            def body(i):
                for u in range(U):
                    at = i * U + u
                    value = tile(step, j, j + 1, at, (j, lax.rem(j + 2, J)))
                    if step < STEPS:
                        grids[step][j + 1, 1 + at, inside] = value
                        y_out[step, 0, j + 1, pl.ds(at, 1), :] = value[0:1]
                        y_out[step, 1, j + 1, pl.ds(at, 1), :] = value[K - 1 : K]
                    else:
                        final[j, at] = value

            loop(0, I // U, body)

        loop(low, high, row)

    def faces(step):
        V = pieces_of(I, (2,))

        def body(i):
            for v in range(V):
                at = i * V + v
                for way in (0, 1):
                    kept = out_at[way]
                    value = tile(step, out_plane[way], kept, at, ((J - 1, 2)[way],))
                    if step < STEPS:
                        grids[step][kept, 1 + at, inside] = value
                        part[step - 1, way, at] = value
                    else:
                        final[out_plane[way], at] = value

        loop(0, I // V, body)

    def halo(step, way, at):
        value = x_in[step, way, at]
        if step > 0:
            value = value + 0.1 * grids[step - 1][in_at[way], 1 + at, inside]
        return 0.1 * value

    def finish(step):
        def columns(way, low, high, n):
            V = pieces_of(high - low, (2,))

            def body(i):
                for v in range(V):
                    at = low + i * V + v
                    extra = halo(step - 1, way, at)
                    if step < STEPS:
                        grids[step][in_at[way], 1 + at, inside] = (
                            part[step - 1, 1 - way, at] + extra
                        )
                    else:
                        plane, here = in_plane[way], at - segments[n][0]
                        final[plane, at] = final[plane, at] + extra
                        totals[n][here] = totals[n][here] + extra

            loop(0, (high - low) // V, body)

        for part_n, (begin, count) in enumerate(x_parts[step - 1]):
            for way in (0, 1):
                arrived("rows", way, [x_copy(step - 1, way, part_n)])

                @pl.when(has_source["rows"][way])
                def _():
                    if step < STEPS:
                        columns(way, begin, begin + count, 0)
                        return
                    for n, (at, width) in enumerate(segments):
                        low, high = max(at, begin), min(at + width, begin + count)
                        if low < high:
                            columns(way, low, high, n)

    def send_plane(step, low=0, high=2):
        for way in (0, 1):
            count = len(x_parts[step])
            start("rows", way, [x_copy(step, way, n) for n in range(count)[low:high]])

    send_plane(0)
    send_columns(0, (0, 1))

    zero = jnp.zeros((K, L), jnp.float32)
    for way in (0, 1):

        @pl.when(jnp.logical_not(has_source["slabs"][way]))
        def _():
            row = PAD - 1 if way == 0 else PAD + K

            def body(j):
                for step in range(STEPS):
                    for i in range(I):
                        grids[step][j, 1 + i, pl.ds(row, 1), :] = zero[0:1]

            loop(0, J, body)

        @pl.when(jnp.logical_not(has_source["cols"][way]))
        def _():
            def body(j):
                for step in range(STEPS):
                    grids[step][j, 0 if way == 0 else I + 1, inside] = zero

            loop(0, J, body)

    for one in load_field:
        one.wait()
    loop(0, J, functools.partial(keep_rims, 0))
    send_rims(0, (0, 1))
    load_cells.wait()

    for step in range(1, STEPS + 1):
        last = step == STEPS
        if step > 1:
            receive(step - 1, (1,))
            if last and paired:
                interior(step, 1, J // 2)

                @pl.when(first)
                def _():
                    for way in (0, 1):
                        sent("rows", way, [x_copy(step - 1, way, 0)])
                    pl.semaphore_signal(go, inc=1, device_id=partner, device_id_type=MESH)

                interior(step, J // 2, J - 1)
            else:
                interior(step, 1, J - 1)
            if not last:
                send_rims(step, (1,))
                send_columns(step, (1,))
        receive(step - 1, (0, 1) if step == 1 else (0,))
        faces(step)
        if step == STEPS - 1 and paired:

            @pl.when(first)
            def _():
                send_plane(step)

            @pl.when(jnp.logical_not(first))
            def _():
                pl.semaphore_wait(go, 1)
                send_plane(step - 1, 1, 2)
                send_plane(step)

        elif step == STEPS - 2 and paired:
            send_plane(step, 0, 1)

            @pl.when(first)
            def _():
                send_plane(step, 1, 2)

        elif not last:
            send_plane(step)
        if step == 1:
            interior(1, 1, J - 1)
            send_rims(1, (1,))
            send_columns(1, (1,))
        if last:
            for n, (first_at, count) in enumerate(segments):

                def add(here):
                    value = final[0, first_at + here]
                    for j in range(1, J):
                        value = value + final[j, first_at + here]
                    totals[n][here] = value

                loop(0, count, add)
        finish(step)
        if not last:
            loop(0, 2, functools.partial(keep_rims, step))
            send_rims(step, (0,))
            send_columns(step, (0,))

    for step in range(STEPS):
        for way in (0, 1):
            plane = [x_copy(step, way, n) for n in range(len(x_parts[step]))]
            if step == STEPS - 1 and paired:

                @pl.when(first)
                def _():
                    sent("rows", way, plane[1:])

                @pl.when(jnp.logical_not(first))
                def _():
                    sent("rows", way, plane)

            else:
                sent("rows", way, plane)
    for way in (0, 1):
        sent("cols", way, [z_copy(STEPS - 1, way, piece) for piece in (0, 1)])
        sent("slabs", way, [y_copy(STEPS - 1, way, piece) for piece in (0, 1)])


def end_kernel(scale, final, field_end, potential, sums, end_sem, sum_sem):
    J, I = final.shape[0], final.shape[1]
    pieces = sum_sem.shape[0]
    W = I // pieces
    whole = pltpu.make_async_copy(final, field_end, end_sem)
    whole.start()

    def piece(q):
        columns = pl.ds(q * W, W)
        return pltpu.make_async_copy(
            sums.at[:, columns], potential.at[:, columns], sum_sem.at[q]
        )

    @pl.when(lax.axis_index("rows") == 0)
    def _():
        for q in range(pieces):

            def body(i):
                value = final[0, i]
                sums[0, i] = value * scale
                for j in range(1, J):
                    value = value + final[j, i]
                    sums[j, i] = value * scale

            loop(q * W, (q + 1) * W, body)
            piece(q).start()
        for q in range(pieces):
            piece(q).wait()

    whole.wait()


def sum_kernel(scale, at, final, below, _, potential, sums, sem):
    J = final.shape[0]
    W = below.shape[0]

    def piece(i):
        return pltpu.make_async_copy(
            sums.at[:, i], potential.at[:, at + i], sem.at[i]
        )

    @pl.when(lax.axis_index("rows") > 0)
    def _():
        for i in range(W):
            value = below[i]
            for j in range(J):
                value = value + final[j, at + i]
                sums[j, i] = value * scale
            piece(i).start()
        for i in range(W):
            piece(i).wait()


def totals_below(total, n):
    below = lax.ppermute(total, "rows", [(r, r + 1) for r in range(n - 1)])
    reach = 1
    while reach < n - 1:
        below = below + lax.ppermute(
            below, "rows", [(r, r + reach) for r in range(n - reach)]
        )
        reach *= 2
    return below


def solution(mesh):
    sizes = {axis: mesh.shape[axis] for axis in AXES + ("trial",)}

    def on_device(field_values, crowding):
        J, I, K, L = field_values.shape
        widths = [width for _, width in segments_of(I)]
        N = len(widths)
        padded = pltpu.VMEM((J, I + 2, K + 2 * PAD, L), jnp.float32)
        block = jax.ShapeDtypeStruct((J, I, K, L), jnp.float32)
        vector = pl.BlockSpec(memory_space=pltpu.VMEM)
        anywhere = pl.BlockSpec(memory_space=pl.ANY)
        dma = pltpu.SemaphoreType.DMA
        final, *totals = pl.pallas_call(
            functools.partial(march_kernel, sizes),
            out_shape=(pltpu.VMEM((J, I, K, L), jnp.float32),)
            + tuple(pltpu.VMEM((width, K, L), jnp.float32) for width in widths),
            in_specs=[anywhere] * 2,
            out_specs=(vector,) * (1 + N),
            scratch_shapes=[
                padded,
                padded,
                padded,
                pltpu.VMEM((J, I, K, L), jnp.float32),
                pltpu.VMEM((STEPS, 2, I, K, L), jnp.float32),
                pltpu.VMEM((STEPS - 1, 2, I, K, L), jnp.float32),
                pltpu.VMEM((STEPS, 2, J, I, L), jnp.float32),
                pltpu.VMEM((STEPS, 2, J, I, L), jnp.float32),
                dma((STEPS + 2, 2)),
                dma((STEPS + 2, 2)),
                dma((2, 2)),
                dma((STEPS, 2, 2)),
                dma((2, 2)),
                dma((STEPS, 2, 2)),
                dma((3,)),
                pltpu.SemaphoreType.REGULAR,
            ],
            compiler_params=pltpu.CompilerParams(
                collective_id=0,
                has_side_effects=True,
                vmem_limit_bytes=50 * 1024 * 1024,
            ),
        )(field_values, crowding)

        bytes_out = J * I * K * L * 4
        scale = 1.0 / (J * sizes["rows"])
        pieces = pieces_of(I, (4, 2))
        belows = []
        if sizes["rows"] > 1:
            belows = [totals_below(total, sizes["rows"]) for total in totals]
        field_end, potential = pl.pallas_call(
            functools.partial(end_kernel, scale),
            out_shape=(block, block),
            in_specs=[vector],
            out_specs=(anywhere, anywhere),
            scratch_shapes=[pltpu.VMEM((J, I, K, L), jnp.float32), dma, dma((pieces,))],
            compiler_params=pltpu.CompilerParams(vmem_limit_bytes=5 * 1024 * 1024),
            cost_estimate=pl.CostEstimate(
                flops=4 * bytes_out, bytes_accessed=bytes_out, transcendentals=0
            ),
        )(final)
        for (at, width), below in zip(segments_of(I), belows):
            potential = pl.pallas_call(
                functools.partial(sum_kernel, scale, at),
                out_shape=block,
                in_specs=[vector, vector, anywhere],
                out_specs=anywhere,
                scratch_shapes=[
                    pltpu.VMEM((J, width, K, L), jnp.float32),
                    dma((width,)),
                ],
                input_output_aliases={2: 0},
                compiler_params=pltpu.CompilerParams(vmem_limit_bytes=5 * 1024 * 1024),
                cost_estimate=pl.CostEstimate(
                    flops=bytes_out,
                    bytes_accessed=bytes_out * width // I,
                    transcendentals=0,
                ),
            )(final, below, potential)
        return potential, field_end

    spec = P(("trial", "rows"), "cols", "slabs", None)
    return jax.shard_map(
        on_device,
        mesh=mesh,
        in_specs=(spec, spec),
        out_specs=(spec, spec),
        check_vma=False,
    )
```

```python
import functools

import jax
import jax.numpy as jnp
from jax import lax
from jax.experimental import pallas as pl
from jax.experimental.pallas import tpu as pltpu
from jax.sharding import PartitionSpec as P

STEPS = 3
MESH = pl.DeviceIdType.MESH
AXES = ("rows", "cols", "slabs")
PAD = 8


def pieces_of(length, counts):
    for count in counts:
        if length % count == 0:
            return count
    return 1


def segments_of(I):
    if I % 4:
        return ((0, I),)
    return ((0, I // 2), (I // 2, I // 4), (I - I // 4, I // 4))


def cut(I, sixteenths):
    lead = I * sixteenths // 16 if I % 16 == 0 else I - I // 2
    return ((0, lead), (lead, I - lead))


def loop(low, high, body):
    def step(at, _):
        body(at)
        return 0

    lax.fori_loop(low, high, step, 0)


def march_kernel(sizes, field, crowd, final, *refs):
    segments = segments_of(field.shape[1])
    totals, refs = refs[: len(segments)], refs[len(segments) :]
    (
        grid0, grid1, grid2, cells, x_in, part, y_in, y_out,
        x_send, x_recv, z_send, z_recv, y_send, y_recv, load, go,
    ) = refs
    J, I, K, L = field.shape
    grids = (grid0, grid1, grid2)
    x_parts = [((0, I),)] * (STEPS - 2) + [cut(I, 12), cut(I, 11)]
    x_slot = [step + max(step - STEPS + 2, 0) for step in range(STEPS)]
    U = pieces_of(I, (4, 2))
    inside = pl.ds(PAD, K)
    place = {axis: lax.axis_index(axis) for axis in AXES}
    has_target = {}
    has_source = {}
    for axis in AXES:
        later, earlier = place[axis] < sizes[axis] - 1, place[axis] > 0
        has_target[axis] = (later, earlier)
        has_source[axis] = (earlier, later)
    trial = lax.axis_index("trial")
    first = lax.rem(trial, 2) == 0
    paired = sizes["trial"] % 2 == 0 and sizes["rows"] > 1
    partner = {"trial": trial + 1 - 2 * lax.rem(trial, 2)}
    out_plane = (J - 1, 0)
    in_plane = (0, J - 1)
    out_at = (0, 1)
    in_at = (1, 0)
    rows = ((0, 2), (2, J - 2))

    def target(axis, way):
        n = sizes[axis]
        return {axis: lax.rem(place[axis] + (1 if way == 0 else n - 1), n)}

    load_field = [
        pltpu.make_async_copy(
            field.at[j], grid0.at[(j + 1) % J, 1 : I + 1, inside], load.at[n]
        )
        for n, j in ((0, 0), (1, J - 1))
    ] + [
        pltpu.make_async_copy(
            field.at[1 : J - 1], grid0.at[2:J, 1 : I + 1, inside], load.at[2]
        )
    ]
    load_cells = pltpu.make_async_copy(crowd, cells, load.at[3])
    for one in load_field:
        one.start()

    barrier = pltpu.get_barrier_semaphore()
    peers = jnp.int32(1 if paired else 0)
    for axis in AXES:
        if sizes[axis] > 1:
            for way in (0, 1):

                @pl.when(has_target[axis][way])
                def _():
                    pl.semaphore_signal(
                        barrier, inc=1, device_id=target(axis, way), device_id_type=MESH
                    )

                peers = peers + has_source[axis][way].astype(jnp.int32)
    if paired:
        pl.semaphore_signal(barrier, inc=1, device_id=partner, device_id_type=MESH)
    pl.semaphore_wait(barrier, peers)

    def x_copy(step, way, n):
        at, count = x_parts[step][n]
        columns = pl.ds(at, count)
        if step == 0:
            source = grid0.at[out_at[way], pl.ds(1 + at, count), inside]
        else:
            source = part.at[step - 1, way, columns]
        return pltpu.make_async_remote_copy(
            src_ref=source,
            dst_ref=x_in.at[step, way, columns],
            send_sem=x_send.at[x_slot[step] + n, way],
            recv_sem=x_recv.at[x_slot[step] + n, way],
            device_id=target("rows", way),
            device_id_type=MESH,
        )

    def z_copy(step, way, piece):
        column = I - 1 if way == 0 else 0
        halo = 0 if way == 0 else I + 1
        if step == 0:
            at, count = ((0, 1), (1, J - 1))[piece]
            source = field.at[pl.ds((J - 1, 0)[piece], count), column]
        else:
            at, count = rows[piece]
            source = grids[step].at[pl.ds(at, count), 1 + column, inside]
        return pltpu.make_async_remote_copy(
            src_ref=source,
            dst_ref=grids[step].at[pl.ds(at, count), halo, inside],
            send_sem=z_send.at[way, piece],
            recv_sem=z_recv.at[step, way, piece],
            device_id=target("cols", way),
            device_id_type=MESH,
        )

    def y_copy(step, way, piece):
        at, count = rows[piece]
        return pltpu.make_async_remote_copy(
            src_ref=y_out.at[step, 1 - way, pl.ds(at, count)],
            dst_ref=y_in.at[step, way, pl.ds(at, count)],
            send_sem=y_send.at[way, piece],
            recv_sem=y_recv.at[step, way, piece],
            device_id=target("slabs", way),
            device_id_type=MESH,
        )

    def start(axis, way, copies):
        if sizes[axis] > 1:

            @pl.when(has_target[axis][way])
            def _():
                for one in copies:
                    one.start()

    def sent(axis, way, copies):
        if sizes[axis] > 1:

            @pl.when(has_target[axis][way])
            def _():
                for one in copies:
                    one.wait_send()

    def arrived(axis, way, copies):
        if sizes[axis] > 1:

            @pl.when(has_source[axis][way])
            def _():
                for one in copies:
                    one.wait_recv()

    def send_rims(step, pieces):
        for way in (0, 1):
            if step > 0:
                sent("slabs", way, [y_copy(step - 1, way, piece) for piece in pieces])
            start("slabs", way, [y_copy(step, way, piece) for piece in pieces])

    def send_columns(step, pieces):
        for way in (0, 1):
            if step > 0:
                sent("cols", way, [z_copy(step - 1, way, piece) for piece in pieces])
            start("cols", way, [z_copy(step, way, piece) for piece in pieces])

    def receive(step, pieces):
        grid = grids[step]
        for way in (0, 1):
            arrived("slabs", way, [y_copy(step, way, piece) for piece in pieces])
            row = PAD - 1 if way == 0 else PAD + K

            def place_row(j):
                def body(i):
                    for u in range(U):
                        at = i * U + u
                        grid[j, 1 + at, pl.ds(row, 1), :] = y_in[
                            step, way, j, pl.ds(at, 1), :
                        ]

                loop(0, I // U, body)

            @pl.when(has_source["slabs"][way])
            def _():
                for piece in pieces:
                    at, count = rows[piece]
                    loop(at, at + count, place_row)

        for way in (0, 1):
            arrived("cols", way, [z_copy(step, way, piece) for piece in pieces])

    def keep_rims(step, j):
        def body(i):
            for u in range(U):
                at = i * U + u
                for side, row in ((0, PAD), (1, PAD + K - 1)):
                    y_out[step, side, j, pl.ds(at, 1), :] = grids[step][
                        j, 1 + at, pl.ds(row, 1), :
                    ]

        loop(0, I // U, body)

    def tile(step, j, at, i, beside):
        old = grids[step - 1]
        middle = old[at, 1 + i, inside]
        around = (old[at, i, inside] + old[at, 2 + i, inside]) + (
            old[at, 1 + i, pl.ds(PAD - 1, K)] + old[at, 1 + i, pl.ds(PAD + 1, K)]
        )
        for other in beside:
            around = around + old[other, 1 + i, inside]
        return middle * (0.6 - 0.2 * (middle * cells[j, i])) + 0.1 * around

    def interior(step, low, high):
        def row(j):
            def body(i):
                for u in range(U):
                    at = i * U + u
                    value = tile(step, j, j + 1, at, (j, lax.rem(j + 2, J)))
                    if step < STEPS:
                        grids[step][j + 1, 1 + at, inside] = value
                        y_out[step, 0, j + 1, pl.ds(at, 1), :] = value[0:1]
                        y_out[step, 1, j + 1, pl.ds(at, 1), :] = value[K - 1 : K]
                    else:
                        final[j, at] = value

            loop(0, I // U, body)

        loop(low, high, row)

    def faces(step):
        V = pieces_of(I, (2,))

        def body(i):
            for v in range(V):
                at = i * V + v
                for way in (0, 1):
                    kept = out_at[way]
                    value = tile(step, out_plane[way], kept, at, ((J - 1, 2)[way],))
                    if step < STEPS:
                        grids[step][kept, 1 + at, inside] = value
                        part[step - 1, way, at] = value
                    else:
                        final[out_plane[way], at] = value

        loop(0, I // V, body)

    def halo(step, way, at):
        value = x_in[step, way, at]
        if step > 0:
            value = value + 0.1 * grids[step - 1][in_at[way], 1 + at, inside]
        return 0.1 * value

    def finish(step):
        def columns(way, low, high, n):
            V = pieces_of(high - low, (2,))

            def body(i):
                for v in range(V):
                    at = low + i * V + v
                    extra = halo(step - 1, way, at)
                    if step < STEPS:
                        grids[step][in_at[way], 1 + at, inside] = (
                            part[step - 1, 1 - way, at] + extra
                        )
                    else:
                        plane, here = in_plane[way], at - segments[n][0]
                        final[plane, at] = final[plane, at] + extra
                        totals[n][here] = totals[n][here] + extra

            loop(0, (high - low) // V, body)

        for part_n, (begin, count) in enumerate(x_parts[step - 1]):
            for way in (0, 1):
                arrived("rows", way, [x_copy(step - 1, way, part_n)])

                @pl.when(has_source["rows"][way])
                def _():
                    if step < STEPS:
                        columns(way, begin, begin + count, 0)
                        return
                    for n, (at, width) in enumerate(segments):
                        low, high = max(at, begin), min(at + width, begin + count)
                        if low < high:
                            columns(way, low, high, n)

    def send_plane(step, low=0, high=2):
        for way in (0, 1):
            count = len(x_parts[step])
            start("rows", way, [x_copy(step, way, n) for n in range(count)[low:high]])

    for one in load_field[:2]:
        one.wait()
    send_plane(0)
    send_columns(0, (0, 1))
    load_cells.start()

    zero = jnp.zeros((K, L), jnp.float32)
    for way in (0, 1):

        @pl.when(jnp.logical_not(has_source["slabs"][way]))
        def _():
            row = PAD - 1 if way == 0 else PAD + K

            def body(j):
                for step in range(STEPS):
                    for i in range(I):
                        grids[step][j, 1 + i, pl.ds(row, 1), :] = zero[0:1]

            loop(0, J, body)

        @pl.when(jnp.logical_not(has_source["cols"][way]))
        def _():
            def body(j):
                for step in range(STEPS):
                    grids[step][j, 0 if way == 0 else I + 1, inside] = zero

            loop(0, J, body)

    load_field[2].wait()
    loop(0, J, functools.partial(keep_rims, 0))
    send_rims(0, (0, 1))
    load_cells.wait()

    for step in range(1, STEPS + 1):
        last = step == STEPS
        if step > 1:
            receive(step - 1, (1,))
            if last and paired:
                interior(step, 1, J // 2)

                @pl.when(first)
                def _():
                    for way in (0, 1):
                        sent("rows", way, [x_copy(step - 1, way, 0)])
                    pl.semaphore_signal(go, inc=1, device_id=partner, device_id_type=MESH)

                interior(step, J // 2, J - 1)
            else:
                interior(step, 1, J - 1)
            if not last:
                send_rims(step, (1,))
                send_columns(step, (1,))
        receive(step - 1, (0, 1) if step == 1 else (0,))
        faces(step)
        if step == STEPS - 1 and paired:

            @pl.when(first)
            def _():
                send_plane(step)

            @pl.when(jnp.logical_not(first))
            def _():
                pl.semaphore_wait(go, 1)
                send_plane(step - 1, 1, 2)
                send_plane(step)

        elif step == STEPS - 2 and paired:
            send_plane(step, 0, 1)

            @pl.when(first)
            def _():
                send_plane(step, 1, 2)

        elif not last:
            send_plane(step)
        if step == 1:
            interior(1, 1, J - 1)
            send_rims(1, (1,))
            send_columns(1, (1,))
        if last:
            for n, (first_at, count) in enumerate(segments):

                def add(here):
                    value = final[0, first_at + here]
                    for j in range(1, J):
                        value = value + final[j, first_at + here]
                    totals[n][here] = value

                loop(0, count, add)
        finish(step)
        if not last:
            loop(0, 2, functools.partial(keep_rims, step))
            send_rims(step, (0,))
            send_columns(step, (0,))

    for step in range(STEPS):
        for way in (0, 1):
            plane = [x_copy(step, way, n) for n in range(len(x_parts[step]))]
            if step == STEPS - 1 and paired:

                @pl.when(first)
                def _():
                    sent("rows", way, plane[1:])

                @pl.when(jnp.logical_not(first))
                def _():
                    sent("rows", way, plane)

            else:
                sent("rows", way, plane)
    for way in (0, 1):
        sent("cols", way, [z_copy(STEPS - 1, way, piece) for piece in (0, 1)])
        sent("slabs", way, [y_copy(STEPS - 1, way, piece) for piece in (0, 1)])


def end_kernel(scale, final, field_end, potential, sums, end_sem, sum_sem):
    J, I = final.shape[0], final.shape[1]
    pieces = sum_sem.shape[0]
    W = I // pieces
    whole = pltpu.make_async_copy(final, field_end, end_sem)
    whole.start()

    def piece(q):
        columns = pl.ds(q * W, W)
        return pltpu.make_async_copy(
            sums.at[:, columns], potential.at[:, columns], sum_sem.at[q]
        )

    @pl.when(lax.axis_index("rows") == 0)
    def _():
        for q in range(pieces):

            def body(i):
                value = final[0, i]
                sums[0, i] = value * scale
                for j in range(1, J):
                    value = value + final[j, i]
                    sums[j, i] = value * scale

            loop(q * W, (q + 1) * W, body)
            piece(q).start()
        for q in range(pieces):
            piece(q).wait()

    whole.wait()


def sum_kernel(scale, at, final, below, _, potential, sums, sem):
    J = final.shape[0]
    W = below.shape[0]

    def piece(i):
        return pltpu.make_async_copy(
            sums.at[:, i], potential.at[:, at + i], sem.at[i]
        )

    @pl.when(lax.axis_index("rows") > 0)
    def _():
        for i in range(W):
            value = below[i]
            for j in range(J):
                value = value + final[j, at + i]
                sums[j, i] = value * scale
            piece(i).start()
        for i in range(W):
            piece(i).wait()


def totals_below(total, n):
    below = lax.ppermute(total, "rows", [(r, r + 1) for r in range(n - 1)])
    reach = 1
    while reach < n - 1:
        below = below + lax.ppermute(
            below, "rows", [(r, r + reach) for r in range(n - reach)]
        )
        reach *= 2
    return below


def solution(mesh):
    sizes = {axis: mesh.shape[axis] for axis in AXES + ("trial",)}

    def on_device(field_values, crowding):
        J, I, K, L = field_values.shape
        widths = [width for _, width in segments_of(I)]
        N = len(widths)
        padded = pltpu.VMEM((J, I + 2, K + 2 * PAD, L), jnp.float32)
        block = jax.ShapeDtypeStruct((J, I, K, L), jnp.float32)
        vector = pl.BlockSpec(memory_space=pltpu.VMEM)
        anywhere = pl.BlockSpec(memory_space=pl.ANY)
        dma = pltpu.SemaphoreType.DMA
        final, *totals = pl.pallas_call(
            functools.partial(march_kernel, sizes),
            out_shape=(pltpu.VMEM((J, I, K, L), jnp.float32),)
            + tuple(pltpu.VMEM((width, K, L), jnp.float32) for width in widths),
            in_specs=[anywhere] * 2,
            out_specs=(vector,) * (1 + N),
            scratch_shapes=[
                padded,
                padded,
                padded,
                pltpu.VMEM((J, I, K, L), jnp.float32),
                pltpu.VMEM((STEPS, 2, I, K, L), jnp.float32),
                pltpu.VMEM((STEPS - 1, 2, I, K, L), jnp.float32),
                pltpu.VMEM((STEPS, 2, J, I, L), jnp.float32),
                pltpu.VMEM((STEPS, 2, J, I, L), jnp.float32),
                dma((STEPS + 2, 2)),
                dma((STEPS + 2, 2)),
                dma((2, 2)),
                dma((STEPS, 2, 2)),
                dma((2, 2)),
                dma((STEPS, 2, 2)),
                dma((4,)),
                pltpu.SemaphoreType.REGULAR,
            ],
            compiler_params=pltpu.CompilerParams(
                collective_id=0,
                has_side_effects=True,
                vmem_limit_bytes=50 * 1024 * 1024,
            ),
        )(field_values, crowding)

        bytes_out = J * I * K * L * 4
        scale = 1.0 / (J * sizes["rows"])
        pieces = pieces_of(I, (4, 2))
        belows = []
        if sizes["rows"] > 1:
            belows = [totals_below(total, sizes["rows"]) for total in totals]
        field_end, potential = pl.pallas_call(
            functools.partial(end_kernel, scale),
            out_shape=(block, block),
            in_specs=[vector],
            out_specs=(anywhere, anywhere),
            scratch_shapes=[pltpu.VMEM((J, I, K, L), jnp.float32), dma, dma((pieces,))],
            compiler_params=pltpu.CompilerParams(vmem_limit_bytes=5 * 1024 * 1024),
            cost_estimate=pl.CostEstimate(
                flops=4 * bytes_out, bytes_accessed=bytes_out, transcendentals=0
            ),
        )(final)
        for (at, width), below in zip(segments_of(I), belows):
            potential = pl.pallas_call(
                functools.partial(sum_kernel, scale, at),
                out_shape=block,
                in_specs=[vector, vector, anywhere],
                out_specs=anywhere,
                scratch_shapes=[
                    pltpu.VMEM((J, width, K, L), jnp.float32),
                    dma((width,)),
                ],
                input_output_aliases={2: 0},
                compiler_params=pltpu.CompilerParams(vmem_limit_bytes=5 * 1024 * 1024),
                cost_estimate=pl.CostEstimate(
                    flops=bytes_out,
                    bytes_accessed=bytes_out * width // I,
                    transcendentals=0,
                ),
            )(final, below, potential)
        return potential, field_end

    spec = P(("trial", "rows"), "cols", "slabs", None)
    return jax.shard_map(
        on_device,
        mesh=mesh,
        in_specs=(spec, spec),
        out_specs=(spec, spec),
        check_vma=False,
    )
```

```python
import functools

import jax
import jax.numpy as jnp
from jax import lax
from jax.experimental import pallas as pl
from jax.experimental.pallas import tpu as pltpu
from jax.sharding import PartitionSpec as P

STEPS = 3
MESH = pl.DeviceIdType.MESH
AXES = ("rows", "cols", "slabs")
PAD = 8


def pieces_of(length, counts):
    for count in counts:
        if length % count == 0:
            return count
    return 1


def segments_of(I):
    if I % 4:
        return ((0, I),)
    return ((0, I // 2), (I // 2, I // 4), (I - I // 4, I // 4))


def cut(I, sixteenths):
    lead = I * sixteenths // 16 if I % 16 == 0 else I - I // 2
    return ((0, lead), (lead, I - lead))


def loop(low, high, body):
    def step(at, _):
        body(at)
        return 0

    lax.fori_loop(low, high, step, 0)


def march_kernel(sizes, field, crowd, final, *refs):
    segments = segments_of(field.shape[1])
    totals, refs = refs[: len(segments)], refs[len(segments) :]
    (
        grid0, grid1, grid2, cells, x_in, part, y_in, y_out,
        x_send, x_recv, z_send, z_recv, y_send, y_recv, load, go,
    ) = refs
    J, I, K, L = field.shape
    grids = (grid0, grid1, grid2)
    x_parts = [((0, I),)] * (STEPS - 2) + [cut(I, 12), cut(I, 11)]
    x_slot = [step + max(step - STEPS + 2, 0) for step in range(STEPS)]
    U = pieces_of(I, (4, 2))
    inside = pl.ds(PAD, K)
    place = {axis: lax.axis_index(axis) for axis in AXES}
    has_target = {}
    has_source = {}
    for axis in AXES:
        later, earlier = place[axis] < sizes[axis] - 1, place[axis] > 0
        has_target[axis] = (later, earlier)
        has_source[axis] = (earlier, later)
    trial = lax.axis_index("trial")
    first = lax.rem(trial, 2) == 0
    paired = sizes["trial"] % 2 == 0 and sizes["rows"] > 1
    partner = {"trial": trial + 1 - 2 * lax.rem(trial, 2)}
    out_plane = (J - 1, 0)
    in_plane = (0, J - 1)
    out_at = (0, 1)
    in_at = (1, 0)
    rows = ((0, 2), (2, J - 2))

    def lane(axis, way):
        return way if sizes[axis] > 2 else 0

    def target(axis, way):
        n = sizes[axis]
        return {axis: lax.rem(place[axis] + (1 if way == 0 else n - 1), n)}

    load_field = [
        pltpu.make_async_copy(
            field.at[j], grid0.at[(j + 1) % J, 1 : I + 1, inside], load.at[n]
        )
        for n, j in ((0, 0), (1, J - 1))
    ] + [
        pltpu.make_async_copy(
            field.at[1 : J - 1], grid0.at[2:J, 1 : I + 1, inside], load.at[2]
        )
    ]
    load_cells = pltpu.make_async_copy(crowd, cells, load.at[3])
    for one in load_field:
        one.start()

    barrier = pltpu.get_barrier_semaphore()
    peers = jnp.int32(1 if paired else 0)
    for axis in AXES:
        if sizes[axis] > 1:
            for way in (0, 1):

                @pl.when(has_target[axis][way])
                def _():
                    pl.semaphore_signal(
                        barrier, inc=1, device_id=target(axis, way), device_id_type=MESH
                    )

                peers = peers + has_source[axis][way].astype(jnp.int32)
    if paired:
        pl.semaphore_signal(barrier, inc=1, device_id=partner, device_id_type=MESH)
    pl.semaphore_wait(barrier, peers)

    def x_copy(step, way, n):
        at, count = x_parts[step][n]
        columns = pl.ds(at, count)
        if step == 0:
            source = grid0.at[out_at[way], pl.ds(1 + at, count), inside]
        else:
            source = part.at[step - 1, way, columns]
        return pltpu.make_async_remote_copy(
            src_ref=source,
            dst_ref=x_in.at[step, way, columns],
            send_sem=x_send.at[x_slot[step] + n, lane("rows", way)],
            recv_sem=x_recv.at[x_slot[step] + n, lane("rows", way)],
            device_id=target("rows", way),
            device_id_type=MESH,
        )

    def z_copy(step, way, piece):
        column = I - 1 if way == 0 else 0
        halo = 0 if way == 0 else I + 1
        if step == 0:
            at, count = ((0, 1), (1, J - 1))[piece]
            source = field.at[pl.ds((J - 1, 0)[piece], count), column]
        else:
            at, count = rows[piece]
            source = grids[step].at[pl.ds(at, count), 1 + column, inside]
        return pltpu.make_async_remote_copy(
            src_ref=source,
            dst_ref=grids[step].at[pl.ds(at, count), halo, inside],
            send_sem=z_send.at[lane("cols", way), piece],
            recv_sem=z_recv.at[step, lane("cols", way), piece],
            device_id=target("cols", way),
            device_id_type=MESH,
        )

    def y_copy(step, way, piece):
        at, count = rows[piece]
        return pltpu.make_async_remote_copy(
            src_ref=y_out.at[step, 1 - way, pl.ds(at, count)],
            dst_ref=y_in.at[step, way, pl.ds(at, count)],
            send_sem=y_send.at[lane("slabs", way), piece],
            recv_sem=y_recv.at[step, lane("slabs", way), piece],
            device_id=target("slabs", way),
            device_id_type=MESH,
        )

    def start(axis, way, copies):
        if sizes[axis] > 1:

            @pl.when(has_target[axis][way])
            def _():
                for one in copies:
                    one.start()

    def sent(axis, way, copies):
        if sizes[axis] > 1:

            @pl.when(has_target[axis][way])
            def _():
                for one in copies:
                    one.wait_send()

    def arrived(axis, way, copies):
        if sizes[axis] > 1:

            @pl.when(has_source[axis][way])
            def _():
                for one in copies:
                    one.wait_recv()

    def send_rims(step, pieces):
        for way in (0, 1):
            if step > 0:
                sent("slabs", way, [y_copy(step - 1, way, piece) for piece in pieces])
            start("slabs", way, [y_copy(step, way, piece) for piece in pieces])

    def send_columns(step, pieces):
        for way in (0, 1):
            if step > 0:
                sent("cols", way, [z_copy(step - 1, way, piece) for piece in pieces])
            start("cols", way, [z_copy(step, way, piece) for piece in pieces])

    def receive(step, pieces):
        grid = grids[step]
        for way in (0, 1):
            arrived("slabs", way, [y_copy(step, way, piece) for piece in pieces])
            row = PAD - 1 if way == 0 else PAD + K

            def place_row(j):
                def body(i):
                    for u in range(U):
                        at = i * U + u
                        grid[j, 1 + at, pl.ds(row, 1), :] = y_in[
                            step, way, j, pl.ds(at, 1), :
                        ]

                loop(0, I // U, body)

            @pl.when(has_source["slabs"][way])
            def _():
                for piece in pieces:
                    at, count = rows[piece]
                    loop(at, at + count, place_row)

        for way in (0, 1):
            arrived("cols", way, [z_copy(step, way, piece) for piece in pieces])

    def keep_rims(step, j):
        def body(i):
            for u in range(U):
                at = i * U + u
                for side, row in ((0, PAD), (1, PAD + K - 1)):
                    y_out[step, side, j, pl.ds(at, 1), :] = grids[step][
                        j, 1 + at, pl.ds(row, 1), :
                    ]

        loop(0, I // U, body)

    def tile(step, j, at, i, beside):
        old = grids[step - 1]
        middle = old[at, 1 + i, inside]
        around = (old[at, i, inside] + old[at, 2 + i, inside]) + (
            old[at, 1 + i, pl.ds(PAD - 1, K)] + old[at, 1 + i, pl.ds(PAD + 1, K)]
        )
        for other in beside:
            around = around + old[other, 1 + i, inside]
        return middle * (0.6 - 0.2 * (middle * cells[j, i])) + 0.1 * around

    def interior(step, low, high):
        def row(j):
            def body(i):
                for u in range(U):
                    at = i * U + u
                    value = tile(step, j, j + 1, at, (j, lax.rem(j + 2, J)))
                    if step < STEPS:
                        grids[step][j + 1, 1 + at, inside] = value
                        y_out[step, 0, j + 1, pl.ds(at, 1), :] = value[0:1]
                        y_out[step, 1, j + 1, pl.ds(at, 1), :] = value[K - 1 : K]
                    else:
                        final[j, at] = value

            loop(0, I // U, body)

        loop(low, high, row)

    def faces(step):
        V = pieces_of(I, (2,))

        def body(i):
            for v in range(V):
                at = i * V + v
                for way in (0, 1):
                    kept = out_at[way]
                    value = tile(step, out_plane[way], kept, at, ((J - 1, 2)[way],))
                    if step < STEPS:
                        grids[step][kept, 1 + at, inside] = value
                        part[step - 1, way, at] = value
                    else:
                        final[out_plane[way], at] = value

        loop(0, I // V, body)

    def halo(step, way, at):
        value = x_in[step, way, at]
        if step > 0:
            value = value + 0.1 * grids[step - 1][in_at[way], 1 + at, inside]
        return 0.1 * value

    def finish(step):
        def columns(way, low, high, n):
            V = pieces_of(high - low, (2,))

            def body(i):
                for v in range(V):
                    at = low + i * V + v
                    extra = halo(step - 1, way, at)
                    if step < STEPS:
                        grids[step][in_at[way], 1 + at, inside] = (
                            part[step - 1, 1 - way, at] + extra
                        )
                    else:
                        plane, here = in_plane[way], at - segments[n][0]
                        final[plane, at] = final[plane, at] + extra
                        totals[n][here] = totals[n][here] + extra

            loop(0, (high - low) // V, body)

        for part_n, (begin, count) in enumerate(x_parts[step - 1]):
            for way in (0, 1):
                arrived("rows", way, [x_copy(step - 1, way, part_n)])

                @pl.when(has_source["rows"][way])
                def _():
                    if step < STEPS:
                        columns(way, begin, begin + count, 0)
                        return
                    for n, (at, width) in enumerate(segments):
                        low, high = max(at, begin), min(at + width, begin + count)
                        if low < high:
                            columns(way, low, high, n)

    def send_plane(step, low=0, high=2):
        for way in (0, 1):
            count = len(x_parts[step])
            start("rows", way, [x_copy(step, way, n) for n in range(count)[low:high]])

    for one in load_field[:2]:
        one.wait()
    send_plane(0)
    send_columns(0, (0, 1))
    load_cells.start()

    zero = jnp.zeros((K, L), jnp.float32)
    for way in (0, 1):

        @pl.when(jnp.logical_not(has_source["slabs"][way]))
        def _():
            row = PAD - 1 if way == 0 else PAD + K

            def body(j):
                for step in range(STEPS):
                    for i in range(I):
                        grids[step][j, 1 + i, pl.ds(row, 1), :] = zero[0:1]

            loop(0, J, body)

        @pl.when(jnp.logical_not(has_source["cols"][way]))
        def _():
            def body(j):
                for step in range(STEPS):
                    grids[step][j, 0 if way == 0 else I + 1, inside] = zero

            loop(0, J, body)

    load_field[2].wait()
    loop(0, J, functools.partial(keep_rims, 0))
    send_rims(0, (0, 1))
    load_cells.wait()

    for step in range(1, STEPS + 1):
        last = step == STEPS
        if step > 1:
            receive(step - 1, (1,))
            if last and paired:
                interior(step, 1, J // 2)

                @pl.when(first)
                def _():
                    for way in (0, 1):
                        sent("rows", way, [x_copy(step - 1, way, 0)])
                    pl.semaphore_signal(go, inc=1, device_id=partner, device_id_type=MESH)

                interior(step, J // 2, J - 1)
            else:
                interior(step, 1, J - 1)
            if not last:
                send_rims(step, (1,))
                send_columns(step, (1,))
        receive(step - 1, (0, 1) if step == 1 else (0,))
        faces(step)
        if step == STEPS - 1 and paired:

            @pl.when(first)
            def _():
                send_plane(step)

            @pl.when(jnp.logical_not(first))
            def _():
                pl.semaphore_wait(go, 1)
                send_plane(step - 1, 1, 2)
                send_plane(step)

        elif step == STEPS - 2 and paired:
            send_plane(step, 0, 1)

            @pl.when(first)
            def _():
                send_plane(step, 1, 2)

        elif not last:
            send_plane(step)
        if step == 1:
            interior(1, 1, J - 1)
            send_rims(1, (1,))
            send_columns(1, (1,))
        if last:
            for n, (first_at, count) in enumerate(segments):

                def add(here):
                    value = final[0, first_at + here]
                    for j in range(1, J):
                        value = value + final[j, first_at + here]
                    totals[n][here] = value

                loop(0, count, add)
        finish(step)
        if not last:
            loop(0, 2, functools.partial(keep_rims, step))
            send_rims(step, (0,))
            send_columns(step, (0,))

    for step in range(STEPS):
        for way in (0, 1):
            plane = [x_copy(step, way, n) for n in range(len(x_parts[step]))]
            if step == STEPS - 1 and paired:

                @pl.when(first)
                def _():
                    sent("rows", way, plane[1:])

                @pl.when(jnp.logical_not(first))
                def _():
                    sent("rows", way, plane)

            else:
                sent("rows", way, plane)
    for way in (0, 1):
        sent("cols", way, [z_copy(STEPS - 1, way, piece) for piece in (0, 1)])
        sent("slabs", way, [y_copy(STEPS - 1, way, piece) for piece in (0, 1)])


def end_kernel(scale, final, field_end, potential, sums, end_sem, sum_sem):
    J, I = final.shape[0], final.shape[1]
    pieces = sum_sem.shape[0]
    W = I // pieces
    whole = pltpu.make_async_copy(final, field_end, end_sem)
    whole.start()

    def piece(q):
        columns = pl.ds(q * W, W)
        return pltpu.make_async_copy(
            sums.at[:, columns], potential.at[:, columns], sum_sem.at[q]
        )

    @pl.when(lax.axis_index("rows") == 0)
    def _():
        for q in range(pieces):

            def body(i):
                value = final[0, i]
                sums[0, i] = value * scale
                for j in range(1, J):
                    value = value + final[j, i]
                    sums[j, i] = value * scale

            loop(q * W, (q + 1) * W, body)
            piece(q).start()
        for q in range(pieces):
            piece(q).wait()

    whole.wait()


def sum_kernel(scale, at, final, below, _, potential, sums, carry, sem):
    J = final.shape[0]
    W = below.shape[0]

    def piece(j):
        return pltpu.make_async_copy(
            sums.at[j], potential.at[j, at : at + W], sem.at[j]
        )

    @pl.when(lax.axis_index("rows") > 0)
    def _():
        for j in range(J):
            before = below if j == 0 else carry
            for i in range(W):
                value = before[i] + final[j, at + i]
                carry[i] = value
                sums[j, i] = value * scale
            piece(j).start()
        for j in range(J):
            piece(j).wait()


def totals_below(total, n):
    below = lax.ppermute(total, "rows", [(r, r + 1) for r in range(n - 1)])
    reach = 1
    while reach < n - 1:
        below = below + lax.ppermute(
            below, "rows", [(r, r + reach) for r in range(n - reach)]
        )
        reach *= 2
    return below


def solution(mesh):
    sizes = {axis: mesh.shape[axis] for axis in AXES + ("trial",)}

    def on_device(field_values, crowding):
        J, I, K, L = field_values.shape
        widths = [width for _, width in segments_of(I)]
        N = len(widths)
        lanes = {axis: 2 if sizes[axis] > 2 else 1 for axis in AXES}
        padded = pltpu.VMEM((J, I + 2, K + 2 * PAD, L), jnp.float32)
        block = jax.ShapeDtypeStruct((J, I, K, L), jnp.float32)
        vector = pl.BlockSpec(memory_space=pltpu.VMEM)
        anywhere = pl.BlockSpec(memory_space=pl.ANY)
        dma = pltpu.SemaphoreType.DMA
        final, *totals = pl.pallas_call(
            functools.partial(march_kernel, sizes),
            out_shape=(pltpu.VMEM((J, I, K, L), jnp.float32),)
            + tuple(pltpu.VMEM((width, K, L), jnp.float32) for width in widths),
            in_specs=[anywhere] * 2,
            out_specs=(vector,) * (1 + N),
            scratch_shapes=[
                padded,
                padded,
                padded,
                pltpu.VMEM((J, I, K, L), jnp.float32),
                pltpu.VMEM((STEPS, 2, I, K, L), jnp.float32),
                pltpu.VMEM((STEPS - 1, 2, I, K, L), jnp.float32),
                pltpu.VMEM((STEPS, 2, J, I, L), jnp.float32),
                pltpu.VMEM((STEPS, 2, J, I, L), jnp.float32),
                dma((STEPS + 2, lanes["rows"])),
                dma((STEPS + 2, lanes["rows"])),
                dma((lanes["cols"], 2)),
                dma((STEPS, lanes["cols"], 2)),
                dma((lanes["slabs"], 2)),
                dma((STEPS, lanes["slabs"], 2)),
                dma((4,)),
                pltpu.SemaphoreType.REGULAR,
            ],
            compiler_params=pltpu.CompilerParams(
                collective_id=0,
                has_side_effects=True,
                vmem_limit_bytes=50 * 1024 * 1024,
            ),
        )(field_values, crowding)

        bytes_out = J * I * K * L * 4
        scale = 1.0 / (J * sizes["rows"])
        pieces = pieces_of(I, (4, 2))
        belows = []
        if sizes["rows"] > 1:
            belows = [totals_below(total, sizes["rows"]) for total in totals]
        field_end, potential = pl.pallas_call(
            functools.partial(end_kernel, scale),
            out_shape=(block, block),
            in_specs=[vector],
            out_specs=(anywhere, anywhere),
            scratch_shapes=[pltpu.VMEM((J, I, K, L), jnp.float32), dma, dma((pieces,))],
            compiler_params=pltpu.CompilerParams(vmem_limit_bytes=5 * 1024 * 1024),
            cost_estimate=pl.CostEstimate(
                flops=4 * bytes_out, bytes_accessed=bytes_out, transcendentals=0
            ),
        )(final)
        for (at, width), below in zip(segments_of(I), belows):
            potential = pl.pallas_call(
                functools.partial(sum_kernel, scale, at),
                out_shape=block,
                in_specs=[vector, vector, anywhere],
                out_specs=anywhere,
                scratch_shapes=[
                    pltpu.VMEM((J, width, K, L), jnp.float32),
                    pltpu.VMEM((width, K, L), jnp.float32),
                    dma((J,)),
                ],
                input_output_aliases={2: 0},
                compiler_params=pltpu.CompilerParams(vmem_limit_bytes=5 * 1024 * 1024),
                cost_estimate=pl.CostEstimate(
                    flops=bytes_out,
                    bytes_accessed=bytes_out * width // I,
                    transcendentals=0,
                ),
            )(final, below, potential)
        return potential, field_end

    spec = P(("trial", "rows"), "cols", "slabs", None)
    return jax.shard_map(
        on_device,
        mesh=mesh,
        in_specs=(spec, spec),
        out_specs=(spec, spec),
        check_vma=False,
    )
```

```python
import functools

import jax
import jax.numpy as jnp
from jax import lax
from jax.experimental import pallas as pl
from jax.experimental.pallas import tpu as pltpu
from jax.sharding import PartitionSpec as P

STEPS = 3
MESH = pl.DeviceIdType.MESH
AXES = ("rows", "cols", "slabs")
PAD = 8


def pieces_of(length, counts):
    for count in counts:
        if length % count == 0:
            return count
    return 1


def segments_of(I):
    if I % 4:
        return ((0, I),)
    return ((0, I // 2), (I // 2, I // 4), (I - I // 4, I // 4))


def cut(I, sixteenths):
    lead = I * sixteenths // 16 if I % 16 == 0 else I - I // 2
    return ((0, lead), (lead, I - lead))


def loop(low, high, body):
    def step(at, _):
        body(at)
        return 0

    lax.fori_loop(low, high, step, 0)


def march_kernel(sizes, field, crowd, final, *refs):
    segments = segments_of(field.shape[1])
    totals, refs = refs[: len(segments)], refs[len(segments) :]
    (
        grid0, grid1, grid2, cells, x_in, part, y_in, y_out,
        x_send, x_recv, z_send, z_recv, y_send, y_recv, load, go,
    ) = refs
    J, I, K, L = field.shape
    grids = (grid0, grid1, grid2)
    x_parts = [((0, I),)] * (STEPS - 2) + [cut(I, 12), cut(I, 11)]
    x_slot = [step + max(step - STEPS + 2, 0) for step in range(STEPS)]
    U = pieces_of(I, (4, 2))
    inside = pl.ds(PAD, K)
    place = {axis: lax.axis_index(axis) for axis in AXES}
    has_target = {}
    has_source = {}
    for axis in AXES:
        later, earlier = place[axis] < sizes[axis] - 1, place[axis] > 0
        has_target[axis] = (later, earlier)
        has_source[axis] = (earlier, later)
    trial = lax.axis_index("trial")
    first = lax.rem(trial, 2) == 0
    paired = sizes["trial"] % 2 == 0 and sizes["rows"] > 1
    partner = {"trial": trial + 1 - 2 * lax.rem(trial, 2)}
    out_plane = (J - 1, 0)
    in_plane = (0, J - 1)
    out_at = (0, 1)
    in_at = (1, 0)
    rows = ((0, 2), (2, J - 2))

    def target(axis, way):
        n = sizes[axis]
        return {axis: lax.rem(place[axis] + (1 if way == 0 else n - 1), n)}

    load_field = [
        pltpu.make_async_copy(
            field.at[j], grid0.at[(j + 1) % J, 1 : I + 1, inside], load.at[n]
        )
        for n, j in ((0, 0), (1, J - 1))
    ] + [
        pltpu.make_async_copy(
            field.at[1 : J - 1], grid0.at[2:J, 1 : I + 1, inside], load.at[2]
        )
    ]
    load_cells = pltpu.make_async_copy(crowd, cells, load.at[3])

    barrier = pltpu.get_barrier_semaphore()
    peers = jnp.int32(1 if paired else 0)
    for axis in AXES:
        if sizes[axis] > 1:
            for way in (0, 1):

                @pl.when(has_target[axis][way])
                def _():
                    pl.semaphore_signal(
                        barrier, inc=1, device_id=target(axis, way), device_id_type=MESH
                    )

                peers = peers + has_source[axis][way].astype(jnp.int32)
    if paired:
        pl.semaphore_signal(barrier, inc=1, device_id=partner, device_id_type=MESH)
    for one in load_field:
        one.start()
    pl.semaphore_wait(barrier, peers)

    def x_copy(step, way, n):
        at, count = x_parts[step][n]
        columns = pl.ds(at, count)
        if step == 0:
            source = grid0.at[out_at[way], pl.ds(1 + at, count), inside]
        else:
            source = part.at[step - 1, way, columns]
        return pltpu.make_async_remote_copy(
            src_ref=source,
            dst_ref=x_in.at[step, way, columns],
            send_sem=x_send.at[x_slot[step] + n, way],
            recv_sem=x_recv.at[x_slot[step] + n, way],
            device_id=target("rows", way),
            device_id_type=MESH,
        )

    def z_copy(step, way, piece):
        column = I - 1 if way == 0 else 0
        halo = 0 if way == 0 else I + 1
        if step == 0:
            at, count = ((0, 1), (1, J - 1))[piece]
            source = field.at[pl.ds((J - 1, 0)[piece], count), column]
        else:
            at, count = rows[piece]
            source = grids[step].at[pl.ds(at, count), 1 + column, inside]
        return pltpu.make_async_remote_copy(
            src_ref=source,
            dst_ref=grids[step].at[pl.ds(at, count), halo, inside],
            send_sem=z_send.at[way, piece],
            recv_sem=z_recv.at[step, way, piece],
            device_id=target("cols", way),
            device_id_type=MESH,
        )

    def y_copy(step, way, piece):
        at, count = rows[piece]
        return pltpu.make_async_remote_copy(
            src_ref=y_out.at[step, 1 - way, pl.ds(at, count)],
            dst_ref=y_in.at[step, way, pl.ds(at, count)],
            send_sem=y_send.at[way, piece],
            recv_sem=y_recv.at[step, way, piece],
            device_id=target("slabs", way),
            device_id_type=MESH,
        )

    def start(axis, way, copies):
        if sizes[axis] > 1:

            @pl.when(has_target[axis][way])
            def _():
                for one in copies:
                    one.start()

    def sent(axis, way, copies):
        if sizes[axis] > 1:

            @pl.when(has_target[axis][way])
            def _():
                for one in copies:
                    one.wait_send()

    def arrived(axis, way, copies):
        if sizes[axis] > 1:

            @pl.when(has_source[axis][way])
            def _():
                for one in copies:
                    one.wait_recv()

    def send_rims(step, pieces):
        for way in (0, 1):
            if step > 0:
                sent("slabs", way, [y_copy(step - 1, way, piece) for piece in pieces])
            start("slabs", way, [y_copy(step, way, piece) for piece in pieces])

    def send_columns(step, pieces):
        for way in (0, 1):
            if step > 0:
                sent("cols", way, [z_copy(step - 1, way, piece) for piece in pieces])
            start("cols", way, [z_copy(step, way, piece) for piece in pieces])

    def receive(step, pieces):
        grid = grids[step]
        for way in (0, 1):
            arrived("slabs", way, [y_copy(step, way, piece) for piece in pieces])
            row = PAD - 1 if way == 0 else PAD + K

            def place_row(j):
                def body(i):
                    for u in range(U):
                        at = i * U + u
                        grid[j, 1 + at, pl.ds(row, 1), :] = y_in[
                            step, way, j, pl.ds(at, 1), :
                        ]

                loop(0, I // U, body)

            @pl.when(has_source["slabs"][way])
            def _():
                for piece in pieces:
                    at, count = rows[piece]
                    loop(at, at + count, place_row)

        for way in (0, 1):
            arrived("cols", way, [z_copy(step, way, piece) for piece in pieces])

    def keep_rims(step, j):
        def body(i):
            for u in range(U):
                at = i * U + u
                for side, row in ((0, PAD), (1, PAD + K - 1)):
                    y_out[step, side, j, pl.ds(at, 1), :] = grids[step][
                        j, 1 + at, pl.ds(row, 1), :
                    ]

        loop(0, I // U, body)

    def tile(step, j, at, i, beside):
        old = grids[step - 1]
        middle = old[at, 1 + i, inside]
        around = (old[at, i, inside] + old[at, 2 + i, inside]) + (
            old[at, 1 + i, pl.ds(PAD - 1, K)] + old[at, 1 + i, pl.ds(PAD + 1, K)]
        )
        for other in beside:
            around = around + old[other, 1 + i, inside]
        return middle * (0.6 - 0.2 * (middle * cells[j, i])) + 0.1 * around

    def interior(step, low, high):
        def row(j):
            def body(i):
                for u in range(U):
                    at = i * U + u
                    value = tile(step, j, j + 1, at, (j, lax.rem(j + 2, J)))
                    if step < STEPS:
                        grids[step][j + 1, 1 + at, inside] = value
                        y_out[step, 0, j + 1, pl.ds(at, 1), :] = value[0:1]
                        y_out[step, 1, j + 1, pl.ds(at, 1), :] = value[K - 1 : K]
                    else:
                        final[j, at] = value

            loop(0, I // U, body)

        loop(low, high, row)

    def faces(step):
        V = pieces_of(I, (2,))

        def body(i):
            for v in range(V):
                at = i * V + v
                for way in (0, 1):
                    kept = out_at[way]
                    value = tile(step, out_plane[way], kept, at, ((J - 1, 2)[way],))
                    if step < STEPS:
                        grids[step][kept, 1 + at, inside] = value
                        part[step - 1, way, at] = value
                    else:
                        final[out_plane[way], at] = value

        loop(0, I // V, body)

    def halo(step, way, at):
        value = x_in[step, way, at]
        if step > 0:
            value = value + 0.1 * grids[step - 1][in_at[way], 1 + at, inside]
        return 0.1 * value

    def finish(step):
        def columns(way, low, high, n):
            V = pieces_of(high - low, (2,))

            def body(i):
                for v in range(V):
                    at = low + i * V + v
                    extra = halo(step - 1, way, at)
                    if step < STEPS:
                        grids[step][in_at[way], 1 + at, inside] = (
                            part[step - 1, 1 - way, at] + extra
                        )
                    else:
                        plane, here = in_plane[way], at - segments[n][0]
                        final[plane, at] = final[plane, at] + extra
                        totals[n][here] = totals[n][here] + extra

            loop(0, (high - low) // V, body)

        for part_n, (begin, count) in enumerate(x_parts[step - 1]):
            for way in (0, 1):
                arrived("rows", way, [x_copy(step - 1, way, part_n)])

                @pl.when(has_source["rows"][way])
                def _():
                    if step < STEPS:
                        columns(way, begin, begin + count, 0)
                        return
                    for n, (at, width) in enumerate(segments):
                        low, high = max(at, begin), min(at + width, begin + count)
                        if low < high:
                            columns(way, low, high, n)

    def send_plane(step, low=0, high=2):
        for way in (0, 1):
            count = len(x_parts[step])
            start("rows", way, [x_copy(step, way, n) for n in range(count)[low:high]])

    for one in load_field[:2]:
        one.wait()
    send_plane(0)
    send_columns(0, (0, 1))
    load_cells.start()

    zero = jnp.zeros((K, L), jnp.float32)
    for way in (0, 1):

        @pl.when(jnp.logical_not(has_source["slabs"][way]))
        def _():
            row = PAD - 1 if way == 0 else PAD + K

            def body(j):
                for step in range(STEPS):
                    for i in range(I):
                        grids[step][j, 1 + i, pl.ds(row, 1), :] = zero[0:1]

            loop(0, J, body)

        @pl.when(jnp.logical_not(has_source["cols"][way]))
        def _():
            def body(j):
                for step in range(STEPS):
                    grids[step][j, 0 if way == 0 else I + 1, inside] = zero

            loop(0, J, body)

    load_field[2].wait()
    loop(0, J, functools.partial(keep_rims, 0))
    send_rims(0, (0, 1))
    load_cells.wait()

    for step in range(1, STEPS + 1):
        last = step == STEPS
        if step > 1:
            receive(step - 1, (1,))
            if last and paired:
                interior(step, 1, J // 2)

                @pl.when(first)
                def _():
                    for way in (0, 1):
                        sent("rows", way, [x_copy(step - 1, way, 0)])
                    pl.semaphore_signal(go, inc=1, device_id=partner, device_id_type=MESH)

                interior(step, J // 2, J - 1)
            else:
                interior(step, 1, J - 1)
            if not last:
                send_rims(step, (1,))
                send_columns(step, (1,))
        receive(step - 1, (0, 1) if step == 1 else (0,))
        faces(step)
        if step == STEPS - 1 and paired:

            @pl.when(first)
            def _():
                send_plane(step)

            @pl.when(jnp.logical_not(first))
            def _():
                pl.semaphore_wait(go, 1)
                send_plane(step - 1, 1, 2)
                send_plane(step)

        elif step == STEPS - 2 and paired:
            send_plane(step, 0, 1)

            @pl.when(first)
            def _():
                send_plane(step, 1, 2)

        elif not last:
            send_plane(step)
        if step == 1:
            interior(1, 1, J - 1)
            send_rims(1, (1,))
            send_columns(1, (1,))
        if last:
            for n, (first_at, count) in enumerate(segments):

                def add(here):
                    value = final[0, first_at + here]
                    for j in range(1, J):
                        value = value + final[j, first_at + here]
                    totals[n][here] = value

                loop(0, count, add)
        finish(step)
        if not last:
            loop(0, 2, functools.partial(keep_rims, step))
            send_rims(step, (0,))
            send_columns(step, (0,))

    for step in range(STEPS):
        for way in (0, 1):
            plane = [x_copy(step, way, n) for n in range(len(x_parts[step]))]
            if step == STEPS - 1 and paired:

                @pl.when(first)
                def _():
                    sent("rows", way, plane[1:])

                @pl.when(jnp.logical_not(first))
                def _():
                    sent("rows", way, plane)

            else:
                sent("rows", way, plane)
    for way in (0, 1):
        sent("cols", way, [z_copy(STEPS - 1, way, piece) for piece in (0, 1)])
        sent("slabs", way, [y_copy(STEPS - 1, way, piece) for piece in (0, 1)])


def end_kernel(scale, final, field_end, potential, sums, end_sem, sum_sem):
    J, I = final.shape[0], final.shape[1]
    pieces = sum_sem.shape[0]
    W = I // pieces
    whole = pltpu.make_async_copy(final, field_end, end_sem)
    whole.start()

    def piece(q):
        columns = pl.ds(q * W, W)
        return pltpu.make_async_copy(
            sums.at[:, columns], potential.at[:, columns], sum_sem.at[q]
        )

    @pl.when(lax.axis_index("rows") == 0)
    def _():
        for q in range(pieces):

            def body(i):
                value = final[0, i]
                sums[0, i] = value * scale
                for j in range(1, J):
                    value = value + final[j, i]
                    sums[j, i] = value * scale

            loop(q * W, (q + 1) * W, body)
            piece(q).start()
        for q in range(pieces):
            piece(q).wait()

    whole.wait()


def sum_kernel(scale, at, final, below, _, potential, sums, sem):
    J = final.shape[0]
    W = below.shape[0]

    def piece(i):
        return pltpu.make_async_copy(
            sums.at[:, i], potential.at[:, at + i], sem.at[i]
        )

    @pl.when(lax.axis_index("rows") > 0)
    def _():
        for i in range(W):
            value = below[i]
            for j in range(J):
                value = value + final[j, at + i]
                sums[j, i] = value * scale
            piece(i).start()
        for i in range(W):
            piece(i).wait()


def totals_below(total, n):
    below = lax.ppermute(total, "rows", [(r, r + 1) for r in range(n - 1)])
    reach = 1
    while reach < n - 1:
        below = below + lax.ppermute(
            below, "rows", [(r, r + reach) for r in range(n - reach)]
        )
        reach *= 2
    return below


def solution(mesh):
    sizes = {axis: mesh.shape[axis] for axis in AXES + ("trial",)}

    def on_device(field_values, crowding):
        J, I, K, L = field_values.shape
        widths = [width for _, width in segments_of(I)]
        N = len(widths)
        padded = pltpu.VMEM((J, I + 2, K + 2 * PAD, L), jnp.float32)
        block = jax.ShapeDtypeStruct((J, I, K, L), jnp.float32)
        vector = pl.BlockSpec(memory_space=pltpu.VMEM)
        anywhere = pl.BlockSpec(memory_space=pl.ANY)
        dma = pltpu.SemaphoreType.DMA
        final, *totals = pl.pallas_call(
            functools.partial(march_kernel, sizes),
            out_shape=(pltpu.VMEM((J, I, K, L), jnp.float32),)
            + tuple(pltpu.VMEM((width, K, L), jnp.float32) for width in widths),
            in_specs=[anywhere] * 2,
            out_specs=(vector,) * (1 + N),
            scratch_shapes=[
                padded,
                padded,
                padded,
                pltpu.VMEM((J, I, K, L), jnp.float32),
                pltpu.VMEM((STEPS, 2, I, K, L), jnp.float32),
                pltpu.VMEM((STEPS - 1, 2, I, K, L), jnp.float32),
                pltpu.VMEM((STEPS, 2, J, I, L), jnp.float32),
                pltpu.VMEM((STEPS, 2, J, I, L), jnp.float32),
                dma((STEPS + 2, 2)),
                dma((STEPS + 2, 2)),
                dma((2, 2)),
                dma((STEPS, 2, 2)),
                dma((2, 2)),
                dma((STEPS, 2, 2)),
                dma((4,)),
                pltpu.SemaphoreType.REGULAR,
            ],
            compiler_params=pltpu.CompilerParams(
                collective_id=0,
                has_side_effects=True,
                vmem_limit_bytes=50 * 1024 * 1024,
            ),
        )(field_values, crowding)

        bytes_out = J * I * K * L * 4
        scale = 1.0 / (J * sizes["rows"])
        pieces = pieces_of(I, (4, 2))
        belows = []
        if sizes["rows"] > 1:
            belows = [totals_below(total, sizes["rows"]) for total in totals]
        field_end, potential = pl.pallas_call(
            functools.partial(end_kernel, scale),
            out_shape=(block, block),
            in_specs=[vector],
            out_specs=(anywhere, anywhere),
            scratch_shapes=[pltpu.VMEM((J, I, K, L), jnp.float32), dma, dma((pieces,))],
            compiler_params=pltpu.CompilerParams(vmem_limit_bytes=5 * 1024 * 1024),
            cost_estimate=pl.CostEstimate(
                flops=4 * bytes_out, bytes_accessed=bytes_out, transcendentals=0
            ),
        )(final)
        for (at, width), below in zip(segments_of(I), belows):
            potential = pl.pallas_call(
                functools.partial(sum_kernel, scale, at),
                out_shape=block,
                in_specs=[vector, vector, anywhere],
                out_specs=anywhere,
                scratch_shapes=[
                    pltpu.VMEM((J, width, K, L), jnp.float32),
                    dma((width,)),
                ],
                input_output_aliases={2: 0},
                compiler_params=pltpu.CompilerParams(vmem_limit_bytes=5 * 1024 * 1024),
                cost_estimate=pl.CostEstimate(
                    flops=bytes_out,
                    bytes_accessed=bytes_out * width // I,
                    transcendentals=0,
                ),
            )(final, below, potential)
        return potential, field_end

    spec = P(("trial", "rows"), "cols", "slabs", None)
    return jax.shard_map(
        on_device,
        mesh=mesh,
        in_specs=(spec, spec),
        out_specs=(spec, spec),
        check_vma=False,
    )
```
